32 devices in a mesh: ta: 8 (over y, x, core), sa: 4 (over z).
Axes of the slice: x: 2, y: 2, z: 4, core: 2. Of those that a mesh axis runs over, the one named last changes fastest.
Arguments:
- eigenvectors: bfloat16 [8, 256, 2, 3, 4, 384], P('ta', None, None, None, 'sa'), may hold values from -17 to 17
- momenta: int32 [8, 3], replicated, may hold values from -4 to 4
- block_order: int32 [4], replicated, may hold values from 0 to 3, each once
Outputs:
- meson_fields: float32 [8, 16, 64, 8, 128], P(None, 'sa', 'ta')
- slice_norms: float32 [8, 256], P('ta')
The draws below stay inside these ranges and needn't reach their ends.
Inputs may be any that keep to these rules, and one draw needn't show every extreme that they name: block_order names every block once.
All inputs are finite; a program needn't handle non-finite values.
Results may differ from the reference program's by a relative error of at most 0.0018.
Values sent between devices are 32-bit elements; how exact they have to be, the bound alone decides.
A program may use at most 64 MiB of HBM per device.

```python
import math
import jax
import jax.numpy as jnp
from jax import lax

NC = 3
BS = 64
NBLK = 4
P_SIZE = 8
LX = 96
NV = 256
NT = 8
NZ = 4
PLANE = 384


def draw_eigenvectors(key, part):
    gauss_key, rough_key = jax.random.split(jax.random.fold_in(key, 17), 2)
    full_shape = (NT, NV, 2, NC, NZ, PLANE)
    roughness = jax.random.uniform(rough_key, (NT, 1, 1, 1, NZ, PLANE), jnp.float32, 0.7, 1.4)
    height = jnp.arange(NZ, dtype=jnp.float32) / max(NZ - 1, 1)
    rising = jnp.sqrt(1.0 + 2.0 * height).reshape(1, 1, 1, 1, NZ, 1)
    values = jnp.clip(jax.random.normal(gauss_key, full_shape, jnp.float32), -4.0, 4.0)
    return (values * roughness * rising).astype(jnp.bfloat16)


def place_ends(array, key, least, top_value):
    shape = array.shape
    index_at = [jax.random.randint(jax.random.fold_in(key, axis), (), 0, shape[axis]) for axis in range(len(shape))]
    array = array.at[tuple(index_at)].set(least)
    longest = shape.index(max(shape))
    index_at[longest] = (index_at[longest] + 1) % shape[longest]
    return array.at[tuple(index_at)].set(top_value)


def setup_inputs(seed: int = 0) -> dict:
    key_of = jax.random.split(jax.random.key(seed), 4)
    return {
        "eigenvectors": draw_eigenvectors(jax.random.fold_in(key_of[3], 71), 0),
        "momenta": place_ends(jax.random.randint(key_of[1], (P_SIZE, 3), -4, 5), jax.random.fold_in(key_of[1], 1), -4, 4).astype(jnp.int32),
        "block_order": jax.random.permutation(key_of[2], NBLK).astype(jnp.int32),
    }


full_turn = 2.0 * math.pi

def phased_right(blocks, cos_table, sin_table):
    real_part = blocks[:, :, 0].astype(jnp.float32)[None]
    imag_part = blocks[:, :, 1].astype(jnp.float32)[None]
    cos_full = cos_table[:, None, None, None, :]
    sin_full = sin_table[:, None, None, None, :]
    phased_re = (real_part * cos_full + imag_part * sin_full).astype(jnp.bfloat16)
    phased_im = (imag_part * cos_full - real_part * sin_full).astype(jnp.bfloat16)
    first_half = jnp.stack([phased_re, phased_im], axis=3)
    second_half = jnp.stack([phased_im, -phased_re], axis=3)
    right_cols = jnp.stack([first_half, second_half], axis=1)
    return right_cols.reshape(right_cols.shape[0], 2, right_cols.shape[2], right_cols.shape[3], -1)

def reference(eigenvectors, momenta, block_order):
    site_count = NZ * PLANE
    site_index = jnp.arange(site_count, dtype=jnp.int32)
    z_coord = site_index // PLANE
    within_plane = site_index % PLANE
    x_coord = within_plane % LX
    y_coord = within_plane // LX
    phase_index = momenta[:, 0:1] * x_coord[None, :] + momenta[:, 1:2] * y_coord[None, :] + momenta[:, 2:3] * z_coord[None, :]
    phase_index = jnp.mod(phase_index, LX).astype(jnp.int32)
    angles = phase_index.astype(jnp.float32) * (full_turn / LX)
    cosines = jnp.cos(angles)[:, None, :]
    sine_vals = jnp.sin(angles)[:, None, :]
    norm_scale = 1.0 / math.sqrt(2 * NC * NZ * PLANE)

    def one_slice(slab_data):
        blocks = slab_data.reshape(NBLK, BS, 2, NC, site_count)
        ordered = jnp.take(blocks, block_order, axis=0)
        left_rows = ordered.reshape(NBLK, BS, 2 * NC * site_count).astype(jnp.float32)

        def one_momentum(trig_pair):
            right_cols = phased_right(ordered, trig_pair[0], trig_pair[1])[0]
            product = jnp.einsum('ark,cbjk->abrcj', left_rows, right_cols.astype(jnp.float32))
            return product.reshape(NBLK * NBLK, BS, 2 * BS)
        fields = lax.map(one_momentum, (cosines, sine_vals))
        squares = lax.optimization_barrier(jnp.sum(jnp.square(slab_data.astype(jnp.float32)), axis=(1, 2, 3, 4)))
        return (fields, squares)
    fields, squares = lax.map(one_slice, eigenvectors)
    meson_fields = jnp.transpose(fields, (1, 2, 3, 0, 4)) * norm_scale
    slice_norms = squares / (2 * NC * NZ * PLANE)
    return (meson_fields, slice_norms)
```

```python
import functools
import math

import jax
import jax.numpy as jnp
from jax import lax
from jax.experimental import pallas as pl
from jax.experimental.pallas import tpu as pltpu
from jax.sharding import PartitionSpec as P

NC = 3
BS = 64
NBLK = 4
LX = 96
MESH = pl.DeviceIdType.MESH

full_turn = 2.0 * math.pi


def kernel(
    n, nta, scale, inv_count,
    order_ref, cos_ref, sin_ref, ev_ref,
    out_ref, norm_ref,
    left, right, parts, rbuf, lbuf, final, recv, nbuf,
    rsend, rrecv, lsend, lrecv, asend, arecv, nsend, nrecv,
):
    t, z = lax.axis_index("ta"), lax.axis_index("sa")
    moms, planes = cos_ref.shape
    ppd = NBLK * NBLK // n
    rows = BS // nta
    half = NC * planes

    barrier = pltpu.get_barrier_semaphore()
    for j in range(1, n):
        pl.semaphore_signal(barrier, inc=1, device_id={"sa": lax.rem(z + j, n)}, device_id_type=MESH)
    for j in range(1, nta):
        pl.semaphore_signal(barrier, inc=1, device_id={"ta": lax.rem(t + j, nta)}, device_id_type=MESH)

    for b in range(NBLK):
        stored = order_ref[b]
        for k in range(2 * NC):
            left[b * BS:(b + 1) * BS, k * planes:(k + 1) * planes] = ev_ref[stored, k]
    squares = []
    for b in range(NBLK):
        total = jnp.zeros((BS, 128), jnp.float32)
        for k in range(2 * NC):
            for lane in range(0, planes, 128):
                value = ev_ref[b, k, :, lane:lane + 128].astype(jnp.float32)
                total = total + value * value
        squares.append(total)
    nbuf[z] = lax.dot_general(
        jnp.ones((8, 128), jnp.float32), jnp.concatenate(squares, axis=0), (((1,), (1,)), ((), ())),
        precision=lax.Precision.HIGHEST, preferred_element_type=jnp.float32,
    )

    pl.semaphore_wait(barrier, n - 1 + nta - 1)

    def norm_copy(peer, slot):
        return pltpu.make_async_remote_copy(
            src_ref=nbuf.at[slot], dst_ref=nbuf.at[slot], send_sem=nsend.at[peer], recv_sem=nrecv.at[slot],
            device_id={"sa": peer}, device_id_type=MESH,
        )

    for j in range(1, n):
        norm_copy(lax.rem(z + j, n), z).start()

    def shard(ref, p, s):
        return ref.at[p, pl.ds(s * ppd, ppd)]

    def rightward(src, p, s):
        return pltpu.make_async_remote_copy(
            src_ref=shard(src, p, s), dst_ref=shard(rbuf, p, s), send_sem=rsend.at[p, s], recv_sem=rrecv.at[p, s],
            device_id={"sa": lax.rem(z + 1, n)}, device_id_type=MESH,
        )

    def leftward(src, p, s):
        return pltpu.make_async_remote_copy(
            src_ref=shard(src, p, s), dst_ref=shard(lbuf, p, s), send_sem=lsend.at[p, s], recv_sem=lrecv.at[p, s],
            device_id={"sa": lax.rem(z + n - 1, n)}, device_id_type=MESH,
        )

    def compute(p, carry):
        for c in range(NC):
            lanes = slice(c * planes, (c + 1) * planes)
            upper = slice(half + c * planes, half + (c + 1) * planes)
            cosine = cos_ref[pl.ds(p, 1), :]
            sine = sin_ref[pl.ds(p, 1), :]
            for b in range(NBLK):
                re = left[b * BS:(b + 1) * BS, lanes].astype(jnp.float32)
                im = left[b * BS:(b + 1) * BS, upper].astype(jnp.float32)
                phased_re = (re * cosine + im * sine).astype(jnp.bfloat16)
                phased_im = (im * cosine - re * sine).astype(jnp.bfloat16)
                first = slice(2 * b * BS, (2 * b + 1) * BS)
                second = slice((2 * b + 1) * BS, (2 * b + 2) * BS)
                right[first, lanes] = phased_re
                right[first, upper] = phased_im
                right[second, lanes] = phased_im
                right[second, upper] = -phased_re
        for pair in range(NBLK // 2):
            product = lax.dot_general(
                left[...], right[pair * 4 * BS:(pair + 1) * 4 * BS, :], (((1,), (1,)), ((), ())),
                preferred_element_type=jnp.float32,
            )
            for a in range(NBLK):
                for b in range(2):
                    parts[p, a * NBLK + 2 * pair + b] = product[a * BS:(a + 1) * BS, b * 2 * BS:(b + 1) * 2 * BS]

        @pl.when(z == 0)
        def _():
            for s in range(n - 1, 0, -1):
                rightward(parts, p, s).start()

        @pl.when(z == n - 1)
        def _():
            for s in range(n - 1):
                leftward(parts, p, s).start()

        return carry

    lax.fori_loop(0, moms, compute, 0)

    def rows_copy(p, peer):
        return pltpu.make_async_remote_copy(
            src_ref=final.at[p, peer], dst_ref=recv.at[p, t], send_sem=asend.at[p], recv_sem=arecv.at[p],
            device_id={"ta": peer}, device_id_type=MESH,
        )

    last = jnp.maximum(z - 1, n - 2 - z)

    def step(i, carry):
        p_right = i - (z - 1)
        p_left = i - (n - 2 - z)
        p_final = i - last
        p_out = p_final - 1

        @pl.when((z > 0) & (p_right >= 0) & (p_right < moms))
        def _():
            for s in range(n - 1, 0, -1):
                @pl.when(s > z)
                def _():
                    copy = rightward(rbuf, p_right, s)
                    copy.wait_recv()
                    for k in range(ppd):
                        rbuf[p_right, s * ppd + k] += parts[p_right, s * ppd + k]
                    copy.start()

        @pl.when((z < n - 1) & (p_left >= 0) & (p_left < moms))
        def _():
            for s in range(n - 1):
                @pl.when(s < z)
                def _():
                    copy = leftward(lbuf, p_left, s)
                    copy.wait_recv()
                    for k in range(ppd):
                        lbuf[p_left, s * ppd + k] += parts[p_left, s * ppd + k]
                    copy.start()

        @pl.when((p_final >= 0) & (p_final < moms))
        def _():
            @pl.when(z > 0)
            def _():
                rightward(rbuf, p_final, z).wait_recv()
                for k in range(ppd):
                    parts[p_final, z * ppd + k] += rbuf[p_final, z * ppd + k]

            @pl.when(z < n - 1)
            def _():
                leftward(lbuf, p_final, z).wait_recv()
                for k in range(ppd):
                    parts[p_final, z * ppd + k] += lbuf[p_final, z * ppd + k]

            for k in range(ppd):
                value = parts[p_final, z * ppd + k] * scale
                for peer in range(nta):
                    final[p_final, peer, k] = value[peer * rows:(peer + 1) * rows]
            for j in range(1, nta):
                rows_copy(p_final, lax.rem(t + j, nta)).start()
            recv[p_final, t] = final[p_final, t]

        @pl.when((p_out >= 0) & (p_out < moms))
        def _():
            arrived = recv.at[p_out, pl.ds(0, nta - 1)]
            pltpu.make_async_copy(arrived, arrived, arecv.at[p_out]).wait()
            for source in range(nta):
                for k in range(ppd):
                    out_ref[p_out, k, :, source, :] = recv[p_out, source, k]

        return carry

    lax.fori_loop(0, moms + n - 1, step, 0)

    for j in range(1, n):
        norm_copy(lax.rem(z + j, n), lax.rem(z + j, n)).wait_recv()
    total = nbuf[0]
    for q in range(1, n):
        total = total + nbuf[q]
    norm_ref[...] = total[0:1] * inv_count
    for j in range(1, n):
        norm_copy(lax.rem(z + j, n), z).wait_send()

    def drain(p, carry):
        for s in range(n):
            @pl.when(s > z)
            def _():
                rightward(parts, p, s).wait_send()

            @pl.when(s < z)
            def _():
                leftward(parts, p, s).wait_send()
        sent = final.at[p, pl.ds(0, nta - 1)]
        pltpu.make_async_copy(sent, sent, asend.at[p]).wait()
        return carry

    lax.fori_loop(0, moms, drain, 0)


def body(eigenvectors, momenta, block_order):
    planes = eigenvectors.shape[-1]
    n, nta = lax.axis_size("sa"), lax.axis_size("ta")
    moms = momenta.shape[0]
    nv = eigenvectors.shape[1]
    ppd = NBLK * NBLK // n
    rows = BS // nta
    stored = eigenvectors.reshape(NBLK, BS, 2 * NC, planes).transpose(0, 2, 1, 3)
    site_index = jnp.arange(planes, dtype=jnp.int32)
    phase_index = (
        momenta[:, 0:1] * (site_index % LX)[None, :]
        + momenta[:, 1:2] * (site_index // LX)[None, :]
        + momenta[:, 2:3] * lax.axis_index("sa")
    )
    angles = jnp.mod(phase_index, LX).astype(jnp.float32) * (full_turn / LX)
    count = 2 * NC * n * planes
    f32 = jnp.float32
    vmem = pl.BlockSpec(memory_space=pltpu.VMEM)
    dma = pltpu.SemaphoreType.DMA
    fields, norms = pl.pallas_call(
        functools.partial(kernel, n, nta, 1.0 / math.sqrt(count), 1.0 / count),
        out_shape=(
            jax.ShapeDtypeStruct((moms, ppd, rows, nta, 2 * BS), f32),
            jax.ShapeDtypeStruct((1, nv), f32),
        ),
        in_specs=[pl.BlockSpec(memory_space=pltpu.SMEM), vmem, vmem, vmem],
        out_specs=(vmem, vmem),
        scratch_shapes=[
            pltpu.VMEM((nv, 2 * NC * planes), jnp.bfloat16),
            pltpu.VMEM((2 * nv, 2 * NC * planes), jnp.bfloat16),
            pltpu.VMEM((moms, NBLK * NBLK, BS, 2 * BS), f32),
            pltpu.VMEM((moms, NBLK * NBLK, BS, 2 * BS), f32),
            pltpu.VMEM((moms, NBLK * NBLK, BS, 2 * BS), f32),
            pltpu.VMEM((moms, nta, ppd, rows, 2 * BS), f32),
            pltpu.VMEM((moms, nta, ppd, rows, 2 * BS), f32),
            pltpu.VMEM((n, 8, nv), f32),
            dma((moms, n)), dma((moms, n)), dma((moms, n)), dma((moms, n)),
            dma((moms,)), dma((moms,)), dma((n,)), dma((n,)),
        ],
        compiler_params=pltpu.CompilerParams(collective_id=0, has_side_effects=True),
    )(block_order, jnp.cos(angles), jnp.sin(angles), stored)
    return fields, norms


def solution(mesh):
    return jax.shard_map(
        body,
        mesh=mesh,
        in_specs=(P("ta", None, None, None, "sa", None), P(), P()),
        out_specs=(P(None, "sa", "ta", None, None), P("ta", None)),
        check_vma=False,
    )
```

```python
import functools
import math

import jax
import jax.numpy as jnp
from jax import lax
from jax.experimental import pallas as pl
from jax.experimental.pallas import tpu as pltpu
from jax.sharding import PartitionSpec as P

NC = 3
BS = 64
NBLK = 4
LX = 96
MESH = pl.DeviceIdType.MESH

full_turn = 2.0 * math.pi


def kernel(
    n, nta, scale, inv_count,
    order_ref, momenta_ref, ev_ref,
    out_ref, norm_ref,
    left, right, parts, rbuf, lbuf, final, recv, nbuf,
    rsend, rrecv, lsend, lrecv, asend, arecv, nsend, nrecv,
):
    t, z = lax.axis_index("ta"), lax.axis_index("sa")
    moms, planes = momenta_ref.shape[1], ev_ref.shape[-1]
    ppd = NBLK * NBLK // n
    rows = BS // nta
    half = NC * planes

    barrier = pltpu.get_barrier_semaphore()
    for j in range(1, n):
        pl.semaphore_signal(barrier, inc=1, device_id={"sa": lax.rem(z + j, n)}, device_id_type=MESH)
    for j in range(1, nta):
        pl.semaphore_signal(barrier, inc=1, device_id={"ta": lax.rem(t + j, nta)}, device_id_type=MESH)

    for b in range(NBLK):
        stored = order_ref[b]
        for k in range(2 * NC):
            left[b * BS:(b + 1) * BS, k * planes:(k + 1) * planes] = ev_ref[k, stored]
    def norm_copy(peer, slot):
        return pltpu.make_async_remote_copy(
            src_ref=nbuf.at[slot], dst_ref=nbuf.at[slot], send_sem=nsend.at[peer], recv_sem=nrecv.at[slot],
            device_id={"sa": peer}, device_id_type=MESH,
        )

    def shard(ref, p, s):
        return ref.at[p, pl.ds(s * ppd, ppd)]

    def rightward(src, p, s):
        return pltpu.make_async_remote_copy(
            src_ref=shard(src, p, s), dst_ref=shard(rbuf, p, s), send_sem=rsend.at[p, s], recv_sem=rrecv.at[p, s],
            device_id={"sa": lax.rem(z + 1, n)}, device_id_type=MESH,
        )

    def leftward(src, p, s):
        return pltpu.make_async_remote_copy(
            src_ref=shard(src, p, s), dst_ref=shard(lbuf, p, s), send_sem=lsend.at[p, s], recv_sem=lrecv.at[p, s],
            device_id={"sa": lax.rem(z + n - 1, n)}, device_id_type=MESH,
        )

    def compute(p):
        site = lax.broadcasted_iota(jnp.int32, (1, planes), 1)
        phase_index = (
            momenta_ref[0, p] * lax.rem(site, LX)
            + momenta_ref[1, p] * lax.div(site, LX)
            + momenta_ref[2, p] * z
        )
        angles = jnp.mod(phase_index, LX).astype(jnp.float32) * (full_turn / LX)
        cosine, sine = jnp.cos(angles), jnp.sin(angles)
        for c in range(NC):
            lanes = slice(c * planes, (c + 1) * planes)
            upper = slice(half + c * planes, half + (c + 1) * planes)
            for b in range(NBLK):
                re = left[b * BS:(b + 1) * BS, lanes].astype(jnp.float32)
                im = left[b * BS:(b + 1) * BS, upper].astype(jnp.float32)
                phased_re = (re * cosine + im * sine).astype(jnp.bfloat16)
                phased_im = (im * cosine - re * sine).astype(jnp.bfloat16)
                first = slice(2 * b * BS, (2 * b + 1) * BS)
                second = slice((2 * b + 1) * BS, (2 * b + 2) * BS)
                right[first, lanes] = phased_re
                right[first, upper] = phased_im
                right[second, lanes] = phased_im
                right[second, upper] = -phased_re
        for pair in range(NBLK // 2):
            product = lax.dot_general(
                left[...], right[pair * 4 * BS:(pair + 1) * 4 * BS, :], (((1,), (1,)), ((), ())),
                preferred_element_type=jnp.float32,
            )
            for a in range(NBLK):
                for b in range(2):
                    parts[p, a * NBLK + 2 * pair + b] = product[a * BS:(a + 1) * BS, b * 2 * BS:(b + 1) * 2 * BS]

    def open_lines(p):
        @pl.when(z == 0)
        def _():
            for s in range(n - 1, 0, -1):
                rightward(parts, p, s).start()

        @pl.when(z == n - 1)
        def _():
            for s in range(n - 1):
                leftward(parts, p, s).start()

    def compute_and_open(p, carry):
        compute(p)
        open_lines(p)
        return carry

    compute(0)
    pl.semaphore_wait(barrier, n - 1 + nta - 1)
    open_lines(0)
    lax.fori_loop(1, moms, compute_and_open, 0)

    squares = []
    for b in range(NBLK):
        total = jnp.zeros((BS, 128), jnp.float32)
        for k in range(2 * NC):
            for lane in range(0, planes, 128):
                value = ev_ref[k, b, :, lane:lane + 128].astype(jnp.float32)
                total = total + value * value
        squares.append(total)
    nbuf[z] = lax.dot_general(
        jnp.ones((8, 128), jnp.float32), jnp.concatenate(squares, axis=0), (((1,), (1,)), ((), ())),
        precision=lax.Precision.HIGHEST, preferred_element_type=jnp.float32,
    )

    for j in range(1, n):
        norm_copy(lax.rem(z + j, n), z).start()

    def rows_copy(p, peer):
        return pltpu.make_async_remote_copy(
            src_ref=final.at[p, peer], dst_ref=recv.at[p, t], send_sem=asend.at[p], recv_sem=arecv.at[p],
            device_id={"ta": peer}, device_id_type=MESH,
        )

    last = jnp.maximum(z - 1, n - 2 - z)

    def step(i, carry):
        p_right = i - (z - 1)
        p_left = i - (n - 2 - z)
        p_final = i - last
        p_out = p_final - 1

        @pl.when((z > 0) & (p_right >= 0) & (p_right < moms))
        def _():
            for s in range(n - 1, 0, -1):
                @pl.when(s > z)
                def _():
                    copy = rightward(rbuf, p_right, s)
                    copy.wait_recv()
                    for k in range(ppd):
                        rbuf[p_right, s * ppd + k] += parts[p_right, s * ppd + k]
                    copy.start()

        @pl.when((z < n - 1) & (p_left >= 0) & (p_left < moms))
        def _():
            for s in range(n - 1):
                @pl.when(s < z)
                def _():
                    copy = leftward(lbuf, p_left, s)
                    copy.wait_recv()
                    for k in range(ppd):
                        lbuf[p_left, s * ppd + k] += parts[p_left, s * ppd + k]
                    copy.start()

        @pl.when((p_final >= 0) & (p_final < moms))
        def _():
            @pl.when(z > 0)
            def _():
                rightward(rbuf, p_final, z).wait_recv()
                for k in range(ppd):
                    parts[p_final, z * ppd + k] += rbuf[p_final, z * ppd + k]

            @pl.when(z < n - 1)
            def _():
                leftward(lbuf, p_final, z).wait_recv()
                for k in range(ppd):
                    parts[p_final, z * ppd + k] += lbuf[p_final, z * ppd + k]

            for k in range(ppd):
                value = parts[p_final, z * ppd + k] * scale
                for peer in range(nta):
                    final[p_final, peer, k] = value[peer * rows:(peer + 1) * rows]
            for j in range(1, nta):
                rows_copy(p_final, lax.rem(t + j, nta)).start()
            recv[p_final, t] = final[p_final, t]

        @pl.when((p_out >= 0) & (p_out < moms))
        def _():
            arrived = recv.at[p_out, pl.ds(0, nta - 1)]
            pltpu.make_async_copy(arrived, arrived, arecv.at[p_out]).wait()
            for source in range(nta):
                for k in range(ppd):
                    out_ref[p_out, k, :, source, :] = recv[p_out, source, k]

        return carry

    lax.fori_loop(0, moms + n - 1, step, 0)

    for j in range(1, n):
        norm_copy(lax.rem(z + j, n), lax.rem(z + j, n)).wait_recv()
    total = nbuf[0]
    for q in range(1, n):
        total = total + nbuf[q]
    norm_ref[...] = total[0:1] * inv_count
    for j in range(1, n):
        norm_copy(lax.rem(z + j, n), z).wait_send()

    def drain(p, carry):
        for s in range(n):
            @pl.when(s > z)
            def _():
                rightward(parts, p, s).wait_send()

            @pl.when(s < z)
            def _():
                leftward(parts, p, s).wait_send()
        sent = final.at[p, pl.ds(0, nta - 1)]
        pltpu.make_async_copy(sent, sent, asend.at[p]).wait()
        return carry

    lax.fori_loop(0, moms, drain, 0)


def body(eigenvectors, momenta, block_order):
    planes = eigenvectors.shape[-1]
    n, nta = lax.axis_size("sa"), lax.axis_size("ta")
    moms = momenta.shape[0]
    nv = eigenvectors.shape[1]
    ppd = NBLK * NBLK // n
    rows = BS // nta
    stored = eigenvectors.reshape(NBLK, BS, 2 * NC, planes).transpose(2, 0, 1, 3)
    count = 2 * NC * n * planes
    f32 = jnp.float32
    vmem = pl.BlockSpec(memory_space=pltpu.VMEM)
    smem = pl.BlockSpec(memory_space=pltpu.SMEM)
    dma = pltpu.SemaphoreType.DMA
    fields, norms = pl.pallas_call(
        functools.partial(kernel, n, nta, 1.0 / math.sqrt(count), 1.0 / count),
        out_shape=(
            jax.ShapeDtypeStruct((moms, ppd, rows, nta, 2 * BS), f32),
            jax.ShapeDtypeStruct((1, nv), f32),
        ),
        in_specs=[smem, smem, vmem],
        out_specs=(vmem, vmem),
        scratch_shapes=[
            pltpu.VMEM((nv, 2 * NC * planes), jnp.bfloat16),
            pltpu.VMEM((2 * nv, 2 * NC * planes), jnp.bfloat16),
            pltpu.VMEM((moms, NBLK * NBLK, BS, 2 * BS), f32),
            pltpu.VMEM((moms, NBLK * NBLK, BS, 2 * BS), f32),
            pltpu.VMEM((moms, NBLK * NBLK, BS, 2 * BS), f32),
            pltpu.VMEM((moms, nta, ppd, rows, 2 * BS), f32),
            pltpu.VMEM((moms, nta, ppd, rows, 2 * BS), f32),
            pltpu.VMEM((n, 8, nv), f32),
            dma((moms, n)), dma((moms, n)), dma((moms, n)), dma((moms, n)),
            dma((moms,)), dma((moms,)), dma((n,)), dma((n,)),
        ],
        compiler_params=pltpu.CompilerParams(collective_id=0, has_side_effects=True, vmem_limit_bytes=30 * 1024 * 1024),
    )(block_order, momenta.T, stored)
    return fields, norms


def solution(mesh):
    return jax.shard_map(
        body,
        mesh=mesh,
        in_specs=(P("ta", None, None, None, "sa", None), P(), P()),
        out_specs=(P(None, "sa", "ta", None, None), P("ta", None)),
        check_vma=False,
    )
```

```python
import functools
import math

import jax
import jax.numpy as jnp
from jax import lax
from jax.experimental import pallas as pl
from jax.experimental.pallas import tpu as pltpu
from jax.sharding import PartitionSpec as P

NC = 3
BS = 64
NBLK = 4
LX = 96
MESH = pl.DeviceIdType.MESH

full_turn = 2.0 * math.pi


def kernel(
    n, nta, scale, inv_count,
    order_ref, momenta_ref, ev_ref,
    out_ref, norm_ref,
    left, right, parts, rbuf, lbuf, final, recv, nbuf,
    rsend, rrecv, lsend, lrecv, asend, arecv, nsend, nrecv,
):
    t, z = lax.axis_index("ta"), lax.axis_index("sa")
    moms, planes = momenta_ref.shape[1], ev_ref.shape[-1]
    ppd = NBLK * NBLK // n
    rows = BS // nta
    half = NC * planes

    barrier = pltpu.get_barrier_semaphore()
    for j in range(1, n):
        pl.semaphore_signal(barrier, inc=1, device_id={"sa": lax.rem(z + j, n)}, device_id_type=MESH)
    for j in range(1, nta):
        pl.semaphore_signal(barrier, inc=1, device_id={"ta": lax.rem(t + j, nta)}, device_id_type=MESH)

    for b in range(NBLK):
        stored = order_ref[b]
        for k in range(2 * NC):
            left[b * BS:(b + 1) * BS, k * planes:(k + 1) * planes] = ev_ref[k, stored]
    def norm_copy(peer, slot):
        return pltpu.make_async_remote_copy(
            src_ref=nbuf.at[slot], dst_ref=nbuf.at[slot], send_sem=nsend.at[peer], recv_sem=nrecv.at[slot],
            device_id={"sa": peer}, device_id_type=MESH,
        )

    def shard(ref, p, s):
        return ref.at[p, pl.ds(s * ppd, ppd)]

    def rightward(src, p, s):
        return pltpu.make_async_remote_copy(
            src_ref=shard(src, p, s), dst_ref=shard(rbuf, p, s), send_sem=rsend.at[p, s], recv_sem=rrecv.at[p, s],
            device_id={"sa": lax.rem(z + 1, n)}, device_id_type=MESH,
        )

    def leftward(src, p, s):
        return pltpu.make_async_remote_copy(
            src_ref=shard(src, p, s), dst_ref=shard(lbuf, p, s), send_sem=lsend.at[p, s], recv_sem=lrecv.at[p, s],
            device_id={"sa": lax.rem(z + n - 1, n)}, device_id_type=MESH,
        )

    def compute(p):
        site = lax.broadcasted_iota(jnp.int32, (1, planes), 1)
        phase_index = (
            momenta_ref[0, p] * lax.rem(site, LX)
            + momenta_ref[1, p] * lax.div(site, LX)
            + momenta_ref[2, p] * z
        )
        angles = jnp.mod(phase_index, LX).astype(jnp.float32) * (full_turn / LX)
        cosine, sine = jnp.cos(angles), jnp.sin(angles)
        for c in range(NC):
            lanes = slice(c * planes, (c + 1) * planes)
            upper = slice(half + c * planes, half + (c + 1) * planes)
            for b in range(NBLK):
                re = left[b * BS:(b + 1) * BS, lanes].astype(jnp.float32)
                im = left[b * BS:(b + 1) * BS, upper].astype(jnp.float32)
                phased_re = (re * cosine + im * sine).astype(jnp.bfloat16)
                phased_im = (im * cosine - re * sine).astype(jnp.bfloat16)
                first = slice(2 * b * BS, (2 * b + 1) * BS)
                second = slice((2 * b + 1) * BS, (2 * b + 2) * BS)
                right[first, lanes] = phased_re
                right[first, upper] = phased_im
                right[second, lanes] = phased_im
                right[second, upper] = -phased_re
        for pair in range(NBLK // 2):
            product = lax.dot_general(
                left[...], right[pair * 4 * BS:(pair + 1) * 4 * BS, :], (((1,), (1,)), ((), ())),
                preferred_element_type=jnp.float32,
            )
            for a in range(NBLK):
                for b in range(2):
                    parts[p, a * NBLK + 2 * pair + b] = product[a * BS:(a + 1) * BS, b * 2 * BS:(b + 1) * 2 * BS]

    def open_lines(slot):
        @pl.when(z == 0)
        def _():
            for s in range(n - 1, 0, -1):
                p = slot - (n - 1 - s)

                @pl.when((p >= 0) & (p < moms))
                def _():
                    rightward(parts, p, s).start()

        @pl.when(z == n - 1)
        def _():
            for s in range(n - 1):
                p = slot - s

                @pl.when((p >= 0) & (p < moms))
                def _():
                    leftward(parts, p, s).start()

    def compute_and_open(p, carry):
        compute(p)
        open_lines(p)
        return carry

    def only_open(slot, carry):
        open_lines(slot)
        return carry

    compute(0)
    pl.semaphore_wait(barrier, n - 1 + nta - 1)
    open_lines(0)
    lax.fori_loop(1, moms, compute_and_open, 0)
    lax.fori_loop(moms, moms + n - 2, only_open, 0)

    squares = []
    for b in range(NBLK):
        total = jnp.zeros((BS, 128), jnp.float32)
        for k in range(2 * NC):
            for lane in range(0, planes, 128):
                value = ev_ref[k, b, :, lane:lane + 128].astype(jnp.float32)
                total = total + value * value
        squares.append(total)
    nbuf[z] = lax.dot_general(
        jnp.ones((8, 128), jnp.float32), jnp.concatenate(squares, axis=0), (((1,), (1,)), ((), ())),
        precision=lax.Precision.HIGHEST, preferred_element_type=jnp.float32,
    )

    for j in range(1, n):
        norm_copy(lax.rem(z + j, n), z).start()

    def rows_copy(p, peer):
        return pltpu.make_async_remote_copy(
            src_ref=final.at[p, peer], dst_ref=recv.at[p, t], send_sem=asend.at[p], recv_sem=arecv.at[p],
            device_id={"ta": peer}, device_id_type=MESH,
        )

    def step(i, carry):
        p_final = i - (n - 2)
        p_out = p_final - 1

        for s in range(n - 1, 0, -1):
            p_right = i - (z - 1) - (n - 1 - s)

            @pl.when((z > 0) & (s > z) & (p_right >= 0) & (p_right < moms))
            def _():
                copy = rightward(rbuf, p_right, s)
                copy.wait_recv()
                for k in range(ppd):
                    rbuf[p_right, s * ppd + k] += parts[p_right, s * ppd + k]
                copy.start()

        for s in range(n - 1):
            p_left = i - (n - 2 - z) - s

            @pl.when((z < n - 1) & (s < z) & (p_left >= 0) & (p_left < moms))
            def _():
                copy = leftward(lbuf, p_left, s)
                copy.wait_recv()
                for k in range(ppd):
                    lbuf[p_left, s * ppd + k] += parts[p_left, s * ppd + k]
                copy.start()

        @pl.when((p_final >= 0) & (p_final < moms))
        def _():
            @pl.when(z > 0)
            def _():
                rightward(rbuf, p_final, z).wait_recv()
                for k in range(ppd):
                    parts[p_final, z * ppd + k] += rbuf[p_final, z * ppd + k]

            @pl.when(z < n - 1)
            def _():
                leftward(lbuf, p_final, z).wait_recv()
                for k in range(ppd):
                    parts[p_final, z * ppd + k] += lbuf[p_final, z * ppd + k]

            for k in range(ppd):
                value = parts[p_final, z * ppd + k] * scale
                for peer in range(nta):
                    final[p_final, peer, k] = value[peer * rows:(peer + 1) * rows]
            for j in range(1, nta):
                rows_copy(p_final, lax.rem(t + j, nta)).start()
            recv[p_final, t] = final[p_final, t]

        @pl.when((p_out >= 0) & (p_out < moms))
        def _():
            arrived = recv.at[p_out, pl.ds(0, nta - 1)]
            pltpu.make_async_copy(arrived, arrived, arecv.at[p_out]).wait()
            for source in range(nta):
                for k in range(ppd):
                    out_ref[p_out, k, :, source, :] = recv[p_out, source, k]

        return carry

    lax.fori_loop(0, moms + n - 1, step, 0)

    for j in range(1, n):
        norm_copy(lax.rem(z + j, n), lax.rem(z + j, n)).wait_recv()
    total = nbuf[0]
    for q in range(1, n):
        total = total + nbuf[q]
    norm_ref[...] = total[0:1] * inv_count
    for j in range(1, n):
        norm_copy(lax.rem(z + j, n), z).wait_send()

    def drain(p, carry):
        for s in range(n):
            @pl.when(s > z)
            def _():
                rightward(parts, p, s).wait_send()

            @pl.when(s < z)
            def _():
                leftward(parts, p, s).wait_send()
        sent = final.at[p, pl.ds(0, nta - 1)]
        pltpu.make_async_copy(sent, sent, asend.at[p]).wait()
        return carry

    lax.fori_loop(0, moms, drain, 0)


def body(eigenvectors, momenta, block_order):
    planes = eigenvectors.shape[-1]
    n, nta = lax.axis_size("sa"), lax.axis_size("ta")
    moms = momenta.shape[0]
    nv = eigenvectors.shape[1]
    ppd = NBLK * NBLK // n
    rows = BS // nta
    stored = eigenvectors.reshape(NBLK, BS, 2 * NC, planes).transpose(2, 0, 1, 3)
    count = 2 * NC * n * planes
    f32 = jnp.float32
    vmem = pl.BlockSpec(memory_space=pltpu.VMEM)
    smem = pl.BlockSpec(memory_space=pltpu.SMEM)
    dma = pltpu.SemaphoreType.DMA
    fields, norms = pl.pallas_call(
        functools.partial(kernel, n, nta, 1.0 / math.sqrt(count), 1.0 / count),
        out_shape=(
            jax.ShapeDtypeStruct((moms, ppd, rows, nta, 2 * BS), f32),
            jax.ShapeDtypeStruct((1, nv), f32),
        ),
        in_specs=[smem, smem, vmem],
        out_specs=(vmem, vmem),
        scratch_shapes=[
            pltpu.VMEM((nv, 2 * NC * planes), jnp.bfloat16),
            pltpu.VMEM((2 * nv, 2 * NC * planes), jnp.bfloat16),
            pltpu.VMEM((moms, NBLK * NBLK, BS, 2 * BS), f32),
            pltpu.VMEM((moms, NBLK * NBLK, BS, 2 * BS), f32),
            pltpu.VMEM((moms, NBLK * NBLK, BS, 2 * BS), f32),
            pltpu.VMEM((moms, nta, ppd, rows, 2 * BS), f32),
            pltpu.VMEM((moms, nta, ppd, rows, 2 * BS), f32),
            pltpu.VMEM((n, 8, nv), f32),
            dma((moms, n)), dma((moms, n)), dma((moms, n)), dma((moms, n)),
            dma((moms,)), dma((moms,)), dma((n,)), dma((n,)),
        ],
        compiler_params=pltpu.CompilerParams(collective_id=0, has_side_effects=True, vmem_limit_bytes=30 * 1024 * 1024),
    )(block_order, momenta.T, stored)
    return fields, norms


def solution(mesh):
    return jax.shard_map(
        body,
        mesh=mesh,
        in_specs=(P("ta", None, None, None, "sa", None), P(), P()),
        out_specs=(P(None, "sa", "ta", None, None), P("ta", None)),
        check_vma=False,
    )
```
